512 devices in a mesh: chan: 128 (over y, z, core), grp: 4 (over x).
Axes of the slice: x: 4, y: 4, z: 16, core: 2. Of those that a mesh axis runs over, the one named last changes fastest.
Arguments:
- eta_pp: bfloat16 [512, 640, 640], P(('chan', 'grp'))
- ham_pp: bfloat16 [512, 640, 640], P(('chan', 'grp'))
- pp_factor: float32 [512, 640], P(('chan', 'grp')), may hold values from -1 to 1
- ph_factor: float32 [512, 640], P(('chan', 'grp')), may hold values from -1 to 1
- channel_size: int32 [512], P(('chan', 'grp')), may hold values from 320 to 640, as said below
- dest_dev: int32 [512, 160], P(('chan', 'grp')), may hold values from 0 to 127, as said below
- dest_sub: int32 [512, 160], P(('chan', 'grp')), may hold values from 0 to 159, as said below
- col_map: int32 [512, 640], P(('chan', 'grp')), may hold values from 0 to 639, each once within a row
- pair_swap: int32 [512, 640], P(('chan', 'grp')), may hold values from 0 to 639, as said below
Outputs:
- pp_flow: float32 [512, 640, 640], P(('chan', 'grp'))
- energy_flow: float32 [], replicated
The draws below stay inside these ranges and needn't reach their ends.
Inputs may be any that keep to these rules, and one draw needn't show every extreme that they name: `channel_size`: a multiple of 4. `dest_dev`: every ph channel receives each of its 160 positions from exactly one pp subblock of its own group; from one pp channel at most 2 subblocks go to one ph channel, and exactly 2 for some. `dest_sub`: for each ph channel the positions it receives are all different. `pair_swap`: an involution of each channel's pairs without fixed points.
All inputs are finite; a program needn't handle non-finite values.
Results may differ from the reference program's by a relative error of at most 0.0036.
Values may be sent and summed in bfloat16 or wider, within the bound.
A program may use at most 64 MiB of HBM per device.

```python
import jax
import jax.numpy as jnp
from jax import lax

CAP = 640
STRIP = 4
SUBS = 160
CHANNELS = 512
N_CHAN = 128
N_GRP = 4


def route_tables(key):
    base = jax.random.fold_in(key, 11)
    key_shift, key_label, key_order = jax.random.split(base, 3)
    shifts = jax.vmap(lambda k: jax.random.permutation(k, N_CHAN))(jax.random.split(key_shift, N_GRP))
    labels = jax.vmap(lambda k: jax.random.permutation(k, N_CHAN))(jax.random.split(key_label, N_GRP))
    orders = jax.vmap(lambda k: jax.random.permutation(k, SUBS))(jax.random.split(key_order, N_CHAN * N_GRP))
    orders = orders.reshape(N_CHAN, N_GRP, SUBS)
    source = jnp.arange(N_CHAN, dtype=jnp.int32)[:, None, None]
    group = jnp.arange(N_GRP, dtype=jnp.int32)[None, :, None]
    block = jnp.arange(SUBS, dtype=jnp.int32)[None, None, :]
    offset = shifts[group, block % N_CHAN]
    targets = labels[group, (source + offset) % N_CHAN]
    position = orders[targets, group, block]
    return (targets.reshape(N_CHAN * N_GRP, SUBS).astype(jnp.int32), position.reshape(N_CHAN * N_GRP, SUBS).astype(jnp.int32))


def draw_dest_dev(key, part):
    return route_tables(key)[0]


def draw_dest_sub(key, part):
    return route_tables(key)[1]


def draw_channel_size(key, part):
    inner = jax.random.fold_in(key, 23)
    counts = jax.random.randint(inner, (N_CHAN * N_GRP,), SUBS // 2, SUBS + 1)
    counts = counts.at[0].set(SUBS).at[1].set(SUBS // 2)
    return (STRIP * counts).astype(jnp.int32)


def draw_pair_swap(key, part):
    inner = jax.random.fold_in(key, 37)

    def involution(k):
        shuffled = jax.random.permutation(k, CAP)
        firsts = shuffled[0::2]
        seconds = shuffled[1::2]
        partner = jnp.zeros((CAP,), jnp.int32).at[firsts].set(seconds)
        return partner.at[seconds].set(firsts)
    return jax.vmap(involution)(jax.random.split(inner, N_CHAN * N_GRP)).astype(jnp.int32)


def factor_rows(key):
    inner = jax.random.fold_in(key, 51)
    return jax.random.uniform(inner, (N_CHAN * N_GRP, CAP), jnp.float32, -1.0, 1.0)


def flow_tables(key, which):
    factors = factor_rows(key)
    inner = jax.random.fold_in(key, 53)
    channel_keys = jax.random.split(inner, N_CHAN * N_GRP)

    def one_channel(args):
        k, factor = args
        key_ham, key_mag = jax.random.split(k)
        raw = jax.random.normal(key_ham, (CAP, CAP), jnp.float32)
        ham = (raw + raw.T) / jnp.sqrt(2.0 * CAP)
        spread = jax.random.uniform(key_mag, (CAP, CAP), jnp.float32, 0.5, 1.5)
        spread = 0.5 * (spread + spread.T)
        direction = jnp.sign(factor[None, :] - factor[:, None])
        gen = spread * ham * direction
        if which == 0:
            return gen.astype(jnp.bfloat16)
        return ham.astype(jnp.bfloat16)
    return lax.map(one_channel, (channel_keys, factors))


def draw_pp_factor(key, part):
    return factor_rows(key)


def draw_eta_pp(key, part):
    return flow_tables(key, 0)


def draw_ham_pp(key, part):
    return flow_tables(key, 1)


def levels(key, shape, shards, least, largest):
    level, own = 1.0, jax.random.fold_in(key, 6)
    for dim, parts in shards:
        draws = jnp.exp(jax.random.uniform(jax.random.fold_in(own, dim), (parts,), jnp.float32, least / len(shards), largest / len(shards)))
        level = level * jnp.repeat(draws, shape[dim] // parts).reshape([-1 if axis == dim else 1 for axis in range(len(shape))])
    return level


def setup_inputs(seed: int = 0) -> dict:
    keys = jax.random.split(jax.random.key(seed), 10)
    return {
        "eta_pp": draw_eta_pp(jax.random.fold_in(keys[9], 71), 0),
        "ham_pp": draw_ham_pp(jax.random.fold_in(keys[9], 71), 0),
        "pp_factor": draw_pp_factor(jax.random.fold_in(keys[9], 71), 0),
        "ph_factor": jnp.clip(jax.random.uniform(keys[3], (CHANNELS, CAP), jnp.float32, -1.0, 1.0) * levels(keys[3], (CHANNELS, CAP), ((0, 512),), -0.4, 0.0), -1.0, 1.0),
        "channel_size": draw_channel_size(jax.random.fold_in(keys[9], 71), 0),
        "dest_dev": draw_dest_dev(jax.random.fold_in(keys[9], 71), 0),
        "dest_sub": draw_dest_sub(jax.random.fold_in(keys[9], 71), 0),
        "col_map": jax.vmap(lambda own: jax.random.permutation(own, CAP))(jax.random.split(keys[7], CHANNELS)).reshape((CHANNELS, CAP)).astype(jnp.int32),
        "pair_swap": draw_pair_swap(jax.random.fold_in(keys[9], 71), 0),
    }


def mask_channel(args):
    gen_block, ham_block, size = args
    pair_index = jnp.arange(CAP, dtype=jnp.int32)
    living = pair_index < size
    inside = living[:, None] & living[None, :]
    zero = jnp.zeros((), jnp.bfloat16)
    return jnp.where(inside, gen_block, zero), jnp.where(inside, ham_block, zero)


def product(left, right):
    return jnp.dot(left.astype(jnp.float32), right.astype(jnp.float32), preferred_element_type=jnp.float32)


def ph_channel(args):
    gen_rows, ham_rows, ph_scale, columns = args
    gen_ph = jnp.take(gen_rows.reshape(CAP, CAP), columns, axis=1)
    ham_ph = jnp.take(ham_rows.reshape(CAP, CAP), columns, axis=1)
    scaled_ham = (ph_scale[:, None] * ham_ph.astype(jnp.float32)).astype(jnp.bfloat16)
    scaled_gen = (ph_scale[:, None] * gen_ph.astype(jnp.float32)).astype(jnp.bfloat16)
    commuted = product(gen_ph, scaled_ham) - product(ham_ph, scaled_gen)
    commuted = commuted.astype(jnp.bfloat16)
    unperm = jnp.zeros((CAP, CAP), jnp.bfloat16).at[:, columns].set(commuted)
    return unperm.reshape(SUBS, STRIP * CAP)


def pp_channel(args):
    gen_m, ham_m, pp_scale, back_rows, partner, size = args
    scaled_ham = (pp_scale[:, None] * ham_m.astype(jnp.float32)).astype(jnp.bfloat16)
    scaled_gen = (pp_scale[:, None] * gen_m.astype(jnp.float32)).astype(jnp.bfloat16)
    ladder = product(gen_m, scaled_ham) - product(ham_m, scaled_gen)
    back = back_rows.reshape(CAP, CAP).astype(jnp.float32)
    anti = back - back[partner, :] - back[:, partner] + back[partner, :][:, partner]
    pair_index = jnp.arange(CAP, dtype=jnp.int32)
    living = pair_index < size
    inside = living[:, None] & living[None, :]
    flow = jnp.where(inside, 0.5 * ladder + anti, jnp.zeros((), jnp.float32))
    return flow, jnp.trace(ladder)


def reference(eta_pp, ham_pp, pp_factor, ph_factor, channel_size, dest_dev, dest_sub, col_map, pair_swap):
    chans = eta_pp.shape[0]
    gen_m, ham_m = lax.map(mask_channel, (eta_pp, ham_pp, channel_size))
    group_of = (jnp.arange(chans, dtype=jnp.int32) % N_GRP).astype(jnp.int32)
    targets = (dest_dev * N_GRP + group_of[:, None]).astype(jnp.int32)
    gen_strips = gen_m.reshape(chans, SUBS, STRIP * CAP)
    ham_strips = ham_m.reshape(chans, SUBS, STRIP * CAP)
    raw_gen = jnp.zeros_like(gen_strips).at[targets, dest_sub].set(gen_strips)
    raw_ham = jnp.zeros_like(ham_strips).at[targets, dest_sub].set(ham_strips)
    ph_back = lax.map(ph_channel, (raw_gen, raw_ham, ph_factor, col_map))
    back = ph_back[targets, dest_sub]
    flow, traces = lax.map(pp_channel, (gen_m, ham_m, pp_factor, back, pair_swap, channel_size))
    energy_flow = 0.25 * jnp.sum(traces)
    return flow, energy_flow
```

```python
import jax
import jax.numpy as jnp
from jax import lax
from jax.experimental import pallas as pl
from jax.experimental.pallas import tpu as pltpu
from jax.sharding import PartitionSpec as P

MESH = pl.DeviceIdType.MESH
HALF = jnp.bfloat16
FULL = jnp.float32
AXES = ("chan", "grp")

PEERS = 128
GROUPS = 4
Y, Z, CORES = 4, 16, 2
PLANE = GROUPS * Y * CORES
CAP = 640
SUBS = 160
STRIP = 4
SLOTS = 2
LINES = SLOTS * STRIP
ROWS = PEERS * LINES
STEP = 256
PART = 320


def dot(left, right):
    return jnp.dot(left, right, preferred_element_type=FULL)


def dot_t(left, right):
    return lax.dot_general(left, right, (((1,), (1,)), ((), ())), preferred_element_type=FULL)


def iota(shape, dim):
    return lax.broadcasted_iota(jnp.int32, shape, dim)


def one_hot(mask):
    return jnp.where(mask, 1.0, 0.0).astype(HALF)


def as_column(row):
    return jnp.transpose(jnp.broadcast_to(row, (128, row.shape[1])))


def at(i, size):
    return pl.ds(pl.multiple_of(i * size, size), size)


def kernel(
    size_ref, gen_ref, ham_ref, pp_ref, ph_ref, dev_ref, sub_ref, cols_ref, swap_ref,
    flow_ref, energy_ref,
    gm, hm, sent, note, got, got_note, left_g, left_h, sc_g, sc_h, mix_g, mix_h,
    ret, got_ret, ladder, column, column_dst, plane_sum, line_sum,
    send_sem, recv_sem, note_send, note_recv, ret_send, ret_recv,
    plane_send, plane_recv, line_send, line_recv,
):
    me = lax.axis_index("chan")
    grp = lax.axis_index("grp")
    my_y, my_z, my_c = me // 32, (me // 2) % 16, me % 2
    seat = grp * 8 + my_y * 2 + my_c

    barrier = pltpu.get_barrier_semaphore()

    def greet(k, carry):
        peer = lax.rem(me + k, PEERS)
        pl.semaphore_signal(barrier, inc=1, device_id={"chan": peer}, device_id_type=MESH)
        return carry

    def greet_plane(k, carry):
        other = lax.rem(grp + 1 + k // 8, GROUPS)
        peer = ((k // 2) % 4) * 32 + my_z * 2 + k % 2
        pl.semaphore_signal(
            barrier, inc=1, device_id={"chan": peer, "grp": other}, device_id_type=MESH
        )
        return carry

    lax.fori_loop(1, PEERS, greet, 0)
    lax.fori_loop(0, 24, greet_plane, 0)

    size = size_ref[0]
    inside = (iota((CAP, CAP), 0) < size) & (iota((CAP, CAP), 1) < size)
    gm[...] = jnp.where(inside, gen_ref[...].astype(FULL), 0.0).astype(HALF)
    hm[...] = jnp.where(inside, ham_ref[...].astype(FULL), 0.0).astype(HALF)

    target = dev_ref[...]
    hits = iota((PEERS, SUBS), 0) == target
    earlier = one_hot(iota((SUBS, SUBS), 0) < iota((SUBS, SUBS), 1))
    count = dot(one_hot(hits), earlier)
    rank = jnp.sum(jnp.where(hits, count, 0.0), axis=0, keepdims=True)
    place = sub_ref[...].astype(FULL) + 1.0
    first = jnp.sum(jnp.where(hits & (rank < 0.5), place, 0.0), axis=1, keepdims=True)
    second = jnp.sum(jnp.where(hits & (rank > 0.5), place, 0.0), axis=1, keepdims=True)
    lane = iota((PEERS, 128), 1)
    notes = jnp.where(lane == 0, first, jnp.where(lane == 1, second, 0.0))
    note[...] = notes.reshape(PEERS, 1, 128)

    slot = (2.0 * target.astype(FULL) + rank).astype(HALF)
    spread = one_hot(iota((SUBS, CAP), 1) // STRIP == iota((SUBS, CAP), 0))
    slots = dot(jnp.broadcast_to(slot, (16, SUBS)), spread)[0:1, :]
    dst = 4.0 * slots + (iota((1, CAP), 1) % STRIP).astype(FULL)
    dst_int = dst.astype(jnp.int32)
    column_dst[...] = as_column(dst).astype(jnp.int32)

    def pack(i, carry):
        pick = one_hot(iota((STEP, CAP), 0) + i * STEP == dst_int)
        g = dot(pick, gm[...]).reshape(STEP // LINES, LINES, CAP)
        h = dot(pick, hm[...]).reshape(STEP // LINES, LINES, CAP)
        sent[pl.ds(i * (STEP // LINES), STEP // LINES)] = jnp.concatenate([g, h], axis=1).astype(HALF)
        return carry

    lax.fori_loop(0, ROWS // STEP, pack, 0)

    pl.semaphore_wait(barrier, PEERS - 1 + 24)

    def send(k, carry):
        peer = lax.rem(me + k, PEERS)
        where = {"chan": peer}
        pltpu.make_async_remote_copy(
            note.at[peer], got_note.at[me], note_send, note_recv,
            device_id=where, device_id_type=MESH,
        ).start()
        pltpu.make_async_remote_copy(
            sent.at[peer], got.at[me], send_sem, recv_sem,
            device_id=where, device_id_type=MESH,
        ).start()
        return carry

    lax.fori_loop(1, PEERS, send, 0)
    got_note[pl.ds(me, 1)] = note[pl.ds(me, 1)]
    got[pl.ds(me, 1)] = sent[pl.ds(me, 1)]

    column[...] = as_column(pp_ref[...])
    sc_g[...] = (column[:, 0:1] * gm[...].astype(FULL)).astype(HALF)
    sc_h[...] = (column[:, 0:1] * hm[...].astype(FULL)).astype(HALF)

    def climb(i, trace):
        rows = at(i, PART)
        part = dot(gm[rows, :], sc_h[...]) - dot(hm[rows, :], sc_g[...])
        ladder[rows, :] = part
        on = iota((PART, CAP), 0) + i * PART == iota((PART, CAP), 1)
        return trace + jnp.sum(jnp.where(on, part, 0.0), axis=0, keepdims=True)

    trace = lax.fori_loop(0, CAP // PART, climb, jnp.zeros((1, CAP), FULL))
    trace = jnp.broadcast_to(jnp.sum(trace, axis=1, keepdims=True), (1, 128))
    plane_sum[pl.ds(seat, 1)] = trace.reshape(1, 1, 128)
    column[...] = as_column(ph_ref[...])

    def share(k, carry):
        @pl.when(k != seat)
        def _():
            pltpu.make_async_remote_copy(
                plane_sum.at[seat], plane_sum.at[seat], plane_send, plane_recv,
                device_id={"chan": ((k // 2) % 4) * 32 + my_z * 2 + k % 2, "grp": k // 8},
                device_id_type=MESH,
            ).start()
        return carry

    lax.fori_loop(0, PLANE, share, 0)

    def drain(ref, count, sem):
        pltpu.make_async_copy(ref.at[pl.ds(0, count)], ref.at[pl.ds(0, count)], sem).wait()

    drain(got_note, PEERS - 1, note_recv)
    flat = got_note[...].reshape(PEERS, 128).astype(HALF)
    r_slot = iota((PEERS, ROWS), 1) // STRIP
    placed = jnp.zeros((16, ROWS), FULL)
    for t in range(SLOTS):
        pick = one_hot(iota((16, 128), 1) == t)
        by_peer = dot_t(pick, flat).astype(HALF)
        placed += dot(by_peer, one_hot(r_slot == SLOTS * iota((PEERS, ROWS), 0) + t))
    source = 4 * (placed[0:1, :].astype(jnp.int32) - 1) + iota((1, ROWS), 1) % STRIP

    drain(got, PEERS - 1, recv_sem)

    def unpack(i, carry):
        block = got[pl.ds(i * (STEP // LINES), STEP // LINES)].astype(FULL)
        rows = at(i, STEP)
        left_g[rows, :] = block[:, 0:LINES, :].reshape(STEP, CAP).astype(HALF)
        left_h[rows, :] = block[:, LINES:, :].reshape(STEP, CAP).astype(HALF)
        return carry

    lax.fori_loop(0, ROWS // STEP, unpack, 0)

    def arrange(i, carry):
        rows = at(i, PART)
        pick = one_hot(iota((PART, ROWS), 0) + i * PART == source)
        scale = column[rows, 0:1]
        sc_g[rows, :] = (scale * dot(pick, left_g[...])).astype(HALF)
        sc_h[rows, :] = (scale * dot(pick, left_h[...])).astype(HALF)
        return carry

    lax.fori_loop(0, CAP // PART, arrange, 0)

    def permute(i, carry):
        rows = at(i, PART)
        pick = one_hot(iota((PART, CAP), 0) + i * PART == cols_ref[...])
        mix_g[rows, :] = dot(pick, sc_g[...]).astype(HALF)
        mix_h[rows, :] = dot(pick, sc_h[...]).astype(HALF)
        return carry

    lax.fori_loop(0, CAP // PART, permute, 0)

    drain(plane_sum, PLANE - 1, plane_recv)
    drain(plane_sum, PLANE - 1, plane_send)
    line_sum[pl.ds(my_z, 1)] = jnp.sum(plane_sum[...], axis=0, keepdims=True)

    def finish(i, carry):
        quarter = lax.rem(i + my_y, Y)
        rows = at(quarter, STEP)
        part = dot(left_g[rows, :], mix_h[...]) - dot(left_h[rows, :], mix_g[...])
        ret[pl.ds(quarter * 32, 32)] = part.reshape(32, LINES, CAP).astype(HALF)
        return carry

    lax.fori_loop(0, ROWS // STEP, finish, 0)

    def along(k, carry):
        peer = my_y * 32 + lax.rem(my_z + k, Z) * 2 + my_c
        pltpu.make_async_remote_copy(
            line_sum.at[my_z], line_sum.at[my_z], line_send, line_recv,
            device_id={"chan": peer}, device_id_type=MESH,
        ).start()
        return carry

    lax.fori_loop(1, Z, along, 0)

    def send_back(k, carry):
        peer = lax.rem(me + k, PEERS)
        pltpu.make_async_remote_copy(
            ret.at[peer], got_ret.at[me], ret_send, ret_recv,
            device_id={"chan": peer}, device_id_type=MESH,
        ).start()
        return carry

    lax.fori_loop(1, PEERS, send_back, 0)
    got_ret[pl.ds(me, 1)] = ret[pl.ds(me, 1)]

    drain(line_sum, Z - 1, line_recv)
    energy_ref[...] = 0.25 * jnp.sum(line_sum[...], axis=0)
    drain(note, PEERS - 1, note_send)
    drain(sent, PEERS - 1, send_sem)
    drain(got_ret, PEERS - 1, ret_recv)

    def unpack_back(i, carry):
        block = got_ret[pl.ds(i * (STEP // LINES), STEP // LINES)].astype(FULL)
        left_g[at(i, STEP), :] = block.reshape(STEP, CAP).astype(HALF)
        return carry

    lax.fori_loop(0, ROWS // STEP, unpack_back, 0)

    def gather(i, carry):
        rows = at(i, PART)
        pick = one_hot(iota((PART, ROWS), 1) == column_dst[rows, 0:1])
        sc_g[rows, :] = dot(pick, left_g[...]).astype(HALF)
        return carry

    lax.fori_loop(0, CAP // PART, gather, 0)
    partner = swap_ref[...]
    mix_g[...] = one_hot(iota((CAP, CAP), 0) == partner)

    def close(i, carry):
        rows = at(i, PART)
        own = sc_g[rows, :]
        swapped = dot(mix_g[rows, :], sc_g[...])
        anti = own.astype(FULL) - swapped - dot(own, mix_g[...]) + dot(swapped.astype(HALF), mix_g[...])
        live = (iota((PART, CAP), 0) + i * PART < size) & (iota((PART, CAP), 1) < size)
        flow_ref[rows, :] = jnp.where(live, 0.5 * ladder[rows, :] + anti, 0.0)
        return carry

    lax.fori_loop(0, CAP // PART, close, 0)
    drain(ret, PEERS - 1, ret_send)
    drain(line_sum, Z - 1, line_send)


def on_device(eta, ham, pp, ph, size, dev, sub, cols, swap):
    vmem = pl.BlockSpec(memory_space=pltpu.VMEM)
    half = lambda *s: pltpu.VMEM(s, HALF)
    full = lambda *s: pltpu.VMEM(s, FULL)
    flow, energy = pl.pallas_call(
        kernel,
        out_shape=(
            jax.ShapeDtypeStruct((CAP, CAP), FULL),
            jax.ShapeDtypeStruct((1, 128), FULL),
        ),
        in_specs=[pl.BlockSpec(memory_space=pltpu.SMEM)] + [vmem] * 8,
        out_specs=(vmem, vmem),
        scratch_shapes=[
            half(CAP, CAP), half(CAP, CAP),
            half(PEERS, 2 * LINES, CAP), full(PEERS, 1, 128),
            half(PEERS, 2 * LINES, CAP), full(PEERS, 1, 128),
            half(ROWS, CAP), half(ROWS, CAP),
            half(CAP, CAP), half(CAP, CAP), half(CAP, CAP), half(CAP, CAP),
            half(PEERS, LINES, CAP), half(PEERS, LINES, CAP),
            full(CAP, CAP), full(CAP, 128), pltpu.VMEM((CAP, 128), jnp.int32),
            full(PLANE, 1, 128), full(Z, 1, 128),
        ] + [pltpu.SemaphoreType.DMA] * 10,
        compiler_params=pltpu.CompilerParams(
            collective_id=0, has_side_effects=True, vmem_limit_bytes=60 << 20
        ),
    )(size, eta[0], ham[0], pp, ph, dev, sub, cols, swap)
    return flow[None], energy[0, 0]


def solution(mesh):
    return jax.shard_map(
        on_device,
        mesh=mesh,
        in_specs=(
            P(AXES, None, None), P(AXES, None, None), P(AXES, None), P(AXES, None), P(AXES),
            P(AXES, None), P(AXES, None), P(AXES, None), P(AXES, None),
        ),
        out_specs=(P(AXES, None, None), P()),
        check_vma=False,
    )
```

```python
import jax
import jax.numpy as jnp
from jax import lax
from jax.experimental import pallas as pl
from jax.experimental.pallas import tpu as pltpu
from jax.sharding import PartitionSpec as P

MESH = pl.DeviceIdType.MESH
HALF = jnp.bfloat16
FULL = jnp.float32
AXES = ("chan", "grp")

PEERS = 128
GROUPS = 4
Y, Z, CORES = 4, 16, 2
PLANE = GROUPS * Y * CORES
CAP = 640
SUBS = 160
STRIP = 4
SLOTS = 2
LINES = SLOTS * STRIP
ROWS = PEERS * LINES
STEP = 256
PART = 320


def dot(left, right):
    return jnp.dot(left, right, preferred_element_type=FULL)


def dot_t(left, right):
    return lax.dot_general(left, right, (((1,), (1,)), ((), ())), preferred_element_type=FULL)


def iota(shape, dim):
    return lax.broadcasted_iota(jnp.int32, shape, dim)


def one_hot(mask):
    return jnp.where(mask, 1.0, 0.0).astype(HALF)


def as_column(row):
    return jnp.transpose(jnp.broadcast_to(row, (128, row.shape[1])))


def at(i, size):
    return pl.ds(pl.multiple_of(i * size, size), size)


def kernel(
    size_ref, gen_hbm, ham_hbm, pp_ref, ph_ref, dev_ref, sub_ref, cols_ref, swap_ref,
    flow_ref, energy_ref,
    gm, hm, sent, note, got, line_note, got_note, left_g, left_h, sc_g, sc_h, mix_g, mix_h,
    forward, backward, acc, both, ret, got_ret, ladder, column, column_dst, plane_sum, line_sum,
    load_sem, send_sem, recv_sem, note_send, note_recv, pass_send, pass_recv, ret_send, ret_recv,
    plane_send, plane_recv, line_send, line_recv,
):
    me = lax.axis_index("chan")
    grp = lax.axis_index("grp")
    my_y, my_z, my_c = me // 32, (me // 2) % 16, me % 2
    spot = my_y * 2 + my_c
    seat = grp * 8 + spot

    loads = [
        pltpu.make_async_copy(gen_hbm, gm, load_sem.at[0]),
        pltpu.make_async_copy(ham_hbm, hm, load_sem.at[1]),
    ]
    for load in loads:
        load.start()
    barrier = pltpu.get_barrier_semaphore()

    def chan_of(y, z, c):
        return lax.rem(y, Y) * 32 + lax.rem(z, Z) * 2 + lax.rem(c, CORES)

    def far_first(k):
        return my_z + 8 + ((k + 1) // 2) * (1 - 2 * (k % 2)) + Z

    def greet(k, carry):
        peer = chan_of(my_y + (k // 2) % 4, far_first(k // 8), my_c + k % 2)

        @pl.when(peer != me)
        def _():
            pl.semaphore_signal(barrier, inc=1, device_id={"chan": peer}, device_id_type=MESH)
        return carry

    def greet_plane(k, carry):
        other = lax.rem(grp + 1 + k // 8, GROUPS)
        peer = chan_of((k // 2) % 4, my_z, k % 2)
        pl.semaphore_signal(
            barrier, inc=1, device_id={"chan": peer, "grp": other}, device_id_type=MESH
        )
        return carry

    lax.fori_loop(0, PEERS, greet, 0)
    lax.fori_loop(0, 24, greet_plane, 0)

    target = dev_ref[...]
    seat_of = (target // 32 * 2 + target % 2) * Z + (target // 2) % Z
    hits = iota((PEERS, SUBS), 0) == seat_of
    earlier = one_hot(iota((SUBS, SUBS), 0) < iota((SUBS, SUBS), 1))
    count = dot(one_hot(hits), earlier)
    rank = jnp.sum(jnp.where(hits, count, 0.0), axis=0, keepdims=True)
    place = sub_ref[...].astype(FULL) + 1.0
    ranks = [
        jnp.sum(jnp.where(hits & (rank < 0.5), place, 0.0), axis=1, keepdims=True),
        jnp.sum(jnp.where(hits & (rank > 0.5), place, 0.0), axis=1, keepdims=True),
    ]
    lane = iota((Z, 128), 1)
    notes = jnp.zeros((Z, 128), FULL)
    for i in range(Y * CORES):
        for t in range(SLOTS):
            notes += jnp.where(lane == SLOTS * i + t, ranks[t][i * Z:(i + 1) * Z, :], 0.0)
    note[...] = notes.reshape(Z, 1, 128)

    slot = (2.0 * target.astype(FULL) + rank).astype(HALF)
    spread = one_hot(iota((SUBS, CAP), 1) // STRIP == iota((SUBS, CAP), 0))
    slots = dot(jnp.broadcast_to(slot, (16, SUBS)), spread)[0:1, :]
    dst = 4.0 * slots + (iota((1, CAP), 1) % STRIP).astype(FULL)
    dst_int = dst.astype(jnp.int32)

    for load in loads:
        load.wait()
    size = size_ref[...]
    inside = (iota((CAP, CAP), 0) < size) & (iota((CAP, CAP), 1) < size)
    gm[...] = jnp.where(inside, gm[...].astype(FULL), 0.0).astype(HALF)
    hm[...] = jnp.where(inside, hm[...].astype(FULL), 0.0).astype(HALF)

    def pack(i, carry):
        pick = one_hot(iota((STEP, CAP), 0) + i * STEP == dst_int)
        g = dot(pick, gm[...]).reshape(STEP // LINES, LINES, CAP)
        h = dot(pick, hm[...]).reshape(STEP // LINES, LINES, CAP)
        sent[pl.ds(i * 32, 32)] = jnp.concatenate([g, h], axis=1).astype(HALF)
        return carry

    lax.fori_loop(0, Y, pack, 0)

    pl.semaphore_wait(barrier, PEERS - 1 + 24)

    def drain(ref, start, count, sem):
        pltpu.make_async_copy(ref.at[pl.ds(start, count)], ref.at[pl.ds(start, count)], sem).wait()

    def send_quarter(src, dst_ref, i, out_sem, in_sem):
        def send(k, carry):
            peer = chan_of(my_y + i, far_first(k // 2), my_c + k % 2)

            def go():
                pltpu.make_async_remote_copy(
                    src.at[peer], dst_ref.at[me], out_sem, in_sem.at[i],
                    device_id={"chan": peer}, device_id_type=MESH,
                ).start()

            if i:
                go()
            else:
                pl.when(peer != me)(go)
            return carry

        lax.fori_loop(0, 32, send, 0)

    def came_from(i):
        return lax.rem(my_y + Y - i, Y)

    def wait_quarter(ref, i, sem):
        if i:
            drain(ref, came_from(i) * 32, 32, sem.at[i])
        else:
            drain(ref, 0, 31, sem.at[i])

    def note_line(k, carry):
        z = lax.rem(my_z + k, Z)
        pltpu.make_async_remote_copy(
            note.at[z], line_note.at[my_z], note_send, note_recv,
            device_id={"chan": chan_of(my_y, z, my_c)}, device_id_type=MESH,
        ).start()
        return carry

    lax.fori_loop(1, Z, note_line, 0)
    line_note[pl.ds(my_z, 1)] = note[pl.ds(my_z, 1)]
    got[pl.ds(me, 1)] = sent[pl.ds(me, 1)]
    send_quarter(sent, got, 0, send_sem, recv_sem)
    drain(line_note, 0, Z - 1, note_recv)

    def note_plane(k, carry):
        other = lax.rem(spot + k, 8)
        pltpu.make_async_remote_copy(
            line_note, got_note.at[spot], pass_send, pass_recv,
            device_id={"chan": chan_of(other // 2, my_z, other % 2)}, device_id_type=MESH,
        ).start()
        return carry

    lax.fori_loop(1, 8, note_plane, 0)
    for i in range(1, Y):
        send_quarter(sent, got, i, send_sem, recv_sem)
    got_note[pl.ds(spot, 1)] = line_note[...].reshape(1, Z, 1, 128)

    column[...] = as_column(pp_ref[...])
    sc_g[...] = (column[:, 0:1] * gm[...].astype(FULL)).astype(HALF)
    sc_h[...] = (column[:, 0:1] * hm[...].astype(FULL)).astype(HALF)

    def climb(i, trace):
        rows = at(i, PART)
        part = dot(gm[rows, :], sc_h[...]) - dot(hm[rows, :], sc_g[...])
        ladder[rows, :] = part
        on = iota((PART, CAP), 0) + i * PART == iota((PART, CAP), 1)
        return trace + jnp.sum(jnp.where(on, part, 0.0), axis=0, keepdims=True)

    trace = lax.fori_loop(0, CAP // PART, climb, jnp.zeros((1, CAP), FULL))
    trace = jnp.broadcast_to(jnp.sum(trace, axis=1, keepdims=True), (1, 128))
    plane_sum[pl.ds(seat, 1)] = trace.reshape(1, 1, 128)

    def share(k, carry):
        @pl.when(k != seat)
        def _():
            pltpu.make_async_remote_copy(
                plane_sum.at[seat], plane_sum.at[seat], plane_send, plane_recv,
                device_id={"chan": chan_of((k // 2) % 4, my_z, k % 2), "grp": k // 8},
                device_id_type=MESH,
            ).start()
        return carry

    lax.fori_loop(0, PLANE, share, 0)

    moved = iota((CAP, CAP), 0) == cols_ref[...]
    mix_g[...] = one_hot(moved)
    scale = jnp.sum(jnp.where(moved, ph_ref[...], 0.0), axis=1, keepdims=True)
    column[...] = jnp.broadcast_to(scale, (CAP, 128))
    swapped = iota((CAP, CAP), 0) == swap_ref[...]
    mix_h[...] = one_hot(swapped)
    dst_swapped = jnp.sum(jnp.where(swapped, dst, 0.0), axis=1, keepdims=True)
    column_dst[0:CAP, :] = as_column(dst).astype(jnp.int32)
    column_dst[CAP:, :] = jnp.broadcast_to(dst_swapped, (CAP, 128)).astype(jnp.int32)
    for q in range(Y):
        backward[q] = one_hot(iota((2 * CAP, STEP), 1) + q * STEP == column_dst[:, 0:1])

    drain(got_note, 0, 7, pass_recv)
    flat = got_note[...].reshape(PEERS, 128).astype(HALF)
    r_peer = iota((PEERS, ROWS), 1) // LINES
    r_seat = (r_peer // 32 * 2 + r_peer % 2) * Z + (r_peer // 2) % Z
    r_slot = iota((PEERS, ROWS), 1) // STRIP % SLOTS
    placed = jnp.zeros((16, ROWS), FULL)
    for t in range(SLOTS):
        pick = one_hot(iota((16, 128), 1) == SLOTS * spot + t)
        by_peer = dot_t(pick, flat).astype(HALF)
        placed += dot(by_peer, one_hot((r_seat == iota((PEERS, ROWS), 0)) & (r_slot == t)))
    source = 4 * (placed[0:1, :].astype(jnp.int32) - 1) + iota((1, ROWS), 1) % STRIP
    for q in range(Y):
        pick = one_hot(iota((CAP, STEP), 0) == source[:, q * STEP:(q + 1) * STEP])
        forward[q] = dot(mix_g[...], pick).astype(HALF)

    for i in range(Y):
        wait_quarter(got, i, recv_sem)
        q = came_from(i)
        block = got[pl.ds(q * 32, 32)].astype(FULL)
        g = block[:, 0:LINES, :].reshape(STEP, CAP).astype(HALF)
        h = block[:, LINES:, :].reshape(STEP, CAP).astype(HALF)
        left_g[at(q, STEP), :] = g
        left_h[at(q, STEP), :] = h
        part_g, part_h = dot(forward[q], g), dot(forward[q], h)
        if i == 0:
            acc[0:CAP, :] = part_g
            acc[CAP:, :] = part_h
        elif i < Y - 1:
            acc[0:CAP, :] += part_g
            acc[CAP:, :] += part_h
        else:
            sc_g[...] = (column[:, 0:1] * (acc[0:CAP, :] + part_g)).astype(HALF)
            sc_h[...] = (column[:, 0:1] * (acc[CAP:, :] + part_h)).astype(HALF)

    for i in range(Y):
        quarter = lax.rem(my_y + i, Y)
        rows = at(quarter, STEP)
        part = dot(left_g[rows, :], sc_h[...]) - dot(left_h[rows, :], sc_g[...])
        ret[pl.ds(quarter * 32, 32)] = part.reshape(32, LINES, CAP).astype(HALF)
        send_quarter(ret, got_ret, i, ret_send, ret_recv)
    got_ret[pl.ds(me, 1)] = ret[pl.ds(me, 1)]

    drain(plane_sum, 0, PLANE - 1, plane_recv)
    drain(plane_sum, 0, PLANE - 1, plane_send)
    line_sum[pl.ds(my_z, 1)] = jnp.sum(plane_sum[...], axis=0, keepdims=True)

    def along(k, carry):
        pltpu.make_async_remote_copy(
            line_sum.at[my_z], line_sum.at[my_z], line_send, line_recv,
            device_id={"chan": chan_of(my_y, my_z + k, my_c)}, device_id_type=MESH,
        ).start()
        return carry

    lax.fori_loop(1, Z, along, 0)

    drain(note, 0, Z - 1, note_send)
    drain(got_note, 0, 7, pass_send)
    drain(sent, 0, PEERS - 1, send_sem)

    for i in range(Y):
        wait_quarter(got_ret, i, ret_recv)
        q = came_from(i)
        block = got_ret[pl.ds(q * 32, 32)].astype(FULL).reshape(STEP, CAP).astype(HALF)
        part = dot(backward[q], block)
        if i == 0:
            acc[...] = part
        elif i < Y - 1:
            acc[...] += part
        else:
            both[...] = (acc[...] + part).astype(HALF)

    def close(i, carry):
        rows = at(i, PART)
        own = both[rows, :]
        other = both[pl.ds(pl.multiple_of(CAP + i * PART, PART), PART), :]
        anti = own.astype(FULL) - other.astype(FULL) - dot(own, mix_h[...]) + dot(other, mix_h[...])
        live = (iota((PART, CAP), 0) + i * PART < size) & (iota((PART, CAP), 1) < size)
        flow_ref[rows, :] = jnp.where(live, 0.5 * ladder[rows, :] + anti, 0.0)
        return carry

    lax.fori_loop(0, CAP // PART, close, 0)
    drain(line_sum, 0, Z - 1, line_recv)
    energy_ref[...] = 0.25 * jnp.sum(line_sum[...], axis=0)
    drain(ret, 0, PEERS - 1, ret_send)
    drain(line_sum, 0, Z - 1, line_send)


def on_device(eta, ham, pp, ph, size, dev, sub, cols, swap):
    vmem = pl.BlockSpec(memory_space=pltpu.VMEM)
    hbm = pl.BlockSpec(memory_space=pl.ANY)
    dma = pltpu.SemaphoreType.DMA
    half = lambda *s: pltpu.VMEM(s, HALF)
    full = lambda *s: pltpu.VMEM(s, FULL)
    flow, energy = pl.pallas_call(
        kernel,
        out_shape=(
            jax.ShapeDtypeStruct((CAP, CAP), FULL),
            jax.ShapeDtypeStruct((1, 128), FULL),
        ),
        in_specs=[vmem, hbm, hbm] + [vmem] * 6,
        out_specs=(vmem, vmem),
        scratch_shapes=[
            half(CAP, CAP), half(CAP, CAP),
            half(PEERS, 2 * LINES, CAP), full(Z, 1, 128),
            half(PEERS, 2 * LINES, CAP), full(Z, 1, 128), full(Y * CORES, Z, 1, 128),
            half(ROWS, CAP), half(ROWS, CAP),
            half(CAP, CAP), half(CAP, CAP), half(CAP, CAP), half(CAP, CAP),
            half(Y, CAP, STEP), half(Y, 2 * CAP, STEP), full(2 * CAP, CAP), half(2 * CAP, CAP),
            half(PEERS, LINES, CAP), half(PEERS, LINES, CAP),
            full(CAP, CAP), full(CAP, 128), pltpu.VMEM((2 * CAP, 128), jnp.int32),
            full(PLANE, 1, 128), full(Z, 1, 128),
            dma((2,)), dma, dma((Y,)), dma, dma, dma, dma, dma, dma((Y,)), dma, dma, dma, dma,
        ],
        compiler_params=pltpu.CompilerParams(
            collective_id=0, has_side_effects=True, vmem_limit_bytes=60 << 20
        ),
    )(size.reshape(1, 1), eta[0], ham[0], pp, ph, dev, sub, cols, swap)
    return flow[None], energy[0, 0]


def solution(mesh):
    return jax.shard_map(
        on_device,
        mesh=mesh,
        in_specs=(
            P(AXES, None, None), P(AXES, None, None), P(AXES, None), P(AXES, None), P(AXES),
            P(AXES, None), P(AXES, None), P(AXES, None), P(AXES, None),
        ),
        out_specs=(P(AXES, None, None), P()),
        check_vma=False,
    )
```

```python
import jax
import jax.numpy as jnp
from jax import lax
from jax.experimental import pallas as pl
from jax.experimental.pallas import tpu as pltpu
from jax.sharding import PartitionSpec as P

MESH = pl.DeviceIdType.MESH
HALF = jnp.bfloat16
FULL = jnp.float32
AXES = ("chan", "grp")

PEERS = 128
GROUPS = 4
Y, Z, CORES = 4, 16, 2
PLANE = GROUPS * Y * CORES
CAP = 640
SUBS = 160
STRIP = 4
SLOTS = 2
LINES = SLOTS * STRIP
ROWS = PEERS * LINES
STEP = 256
PART = 320


def dot(left, right):
    return jnp.dot(left, right, preferred_element_type=FULL)


def dot_t(left, right):
    return lax.dot_general(left, right, (((1,), (1,)), ((), ())), preferred_element_type=FULL)


def iota(shape, dim):
    return lax.broadcasted_iota(jnp.int32, shape, dim)


def one_hot(mask):
    return jnp.where(mask, 1.0, 0.0).astype(HALF)


def as_column(row):
    return jnp.transpose(jnp.broadcast_to(row, (128, row.shape[1])))


def at(i, size):
    return pl.ds(pl.multiple_of(i * size, size), size)


def kernel(
    size_ref, gen_hbm, ham_hbm, pp_ref, ph_ref, dev_ref, sub_ref, cols_ref, swap_ref,
    flow_ref, energy_ref,
    gm, hm, sent, note, got, line_note, got_note, left_g, left_h, sc_g, sc_h, mix_g, mix_h,
    forward, backward, acc, ret, got_ret, column, source, plane_sum, line_sum,
    load_sem, send_sem, recv_sem, note_send, note_recv, pass_send, pass_recv, ret_send, ret_recv,
    plane_send, plane_recv, line_send, line_recv,
):
    me = lax.axis_index("chan")
    grp = lax.axis_index("grp")
    my_y, my_z, my_c = me // 32, (me // 2) % 16, me % 2
    spot = my_y * 2 + my_c
    seat = grp * 8 + spot

    loads = [
        pltpu.make_async_copy(gen_hbm, gm, load_sem.at[0]),
        pltpu.make_async_copy(ham_hbm, hm, load_sem.at[1]),
    ]
    for load in loads:
        load.start()
    barrier = pltpu.get_barrier_semaphore()

    def chan_of(y, z, c):
        return lax.rem(y, Y) * 32 + lax.rem(z, Z) * 2 + lax.rem(c, CORES)

    def far_first(k):
        return my_z + 8 + ((k + 1) // 2) * (1 - 2 * (k % 2)) + Z

    def greet(k, carry):
        peer = chan_of(my_y + (k // 2) % 4, far_first(k // 8), my_c + k % 2)

        @pl.when(peer != me)
        def _():
            pl.semaphore_signal(barrier, inc=1, device_id={"chan": peer}, device_id_type=MESH)
        return carry

    def greet_plane(k, carry):
        other = lax.rem(grp + 1 + k // 8, GROUPS)
        peer = chan_of((k // 2) % 4, my_z, k % 2)
        pl.semaphore_signal(
            barrier, inc=1, device_id={"chan": peer, "grp": other}, device_id_type=MESH
        )
        return carry

    lax.fori_loop(0, PEERS, greet, 0)
    lax.fori_loop(0, 24, greet_plane, 0)

    target = dev_ref[...]
    seat_of = (target // 32 * 2 + target % 2) * Z + (target // 2) % Z
    hits = iota((PEERS, SUBS), 0) == seat_of
    earlier = one_hot(iota((SUBS, SUBS), 0) < iota((SUBS, SUBS), 1))
    count = dot(one_hot(hits), earlier)
    rank = jnp.sum(jnp.where(hits, count, 0.0), axis=0, keepdims=True)
    place = sub_ref[...].astype(FULL) + 1.0
    ranks = [
        jnp.sum(jnp.where(hits & (rank < 0.5), place, 0.0), axis=1, keepdims=True),
        jnp.sum(jnp.where(hits & (rank > 0.5), place, 0.0), axis=1, keepdims=True),
    ]
    lane = iota((Z, 128), 1)
    notes = jnp.zeros((Z, 128), FULL)
    for i in range(Y * CORES):
        for t in range(SLOTS):
            notes += jnp.where(lane == SLOTS * i + t, ranks[t][i * Z:(i + 1) * Z, :], 0.0)
    note[...] = notes.reshape(Z, 1, 128)

    slot = (2.0 * target.astype(FULL) + rank).astype(HALF)
    spread = one_hot(iota((SUBS, CAP), 1) // STRIP == iota((SUBS, CAP), 0))
    slots = dot(jnp.broadcast_to(slot, (16, SUBS)), spread)[0:1, :]
    dst = 4.0 * slots + (iota((1, CAP), 1) % STRIP).astype(FULL)
    dst_int = dst.astype(jnp.int32)

    for load in loads:
        load.wait()
    size = size_ref[0]
    inside = (iota((CAP, CAP), 0) < size) & (iota((CAP, CAP), 1) < size)
    gm[...] = jnp.where(inside, gm[...].astype(FULL), 0.0).astype(HALF)
    hm[...] = jnp.where(inside, hm[...].astype(FULL), 0.0).astype(HALF)

    def pack(i, carry):
        pick = one_hot(iota((STEP, CAP), 0) + i * STEP == dst_int)
        g = dot(pick, gm[...]).reshape(STEP // LINES, LINES, CAP)
        h = dot(pick, hm[...]).reshape(STEP // LINES, LINES, CAP)
        sent[pl.ds(i * 32, 32)] = jnp.concatenate([g, h], axis=1).astype(HALF)
        return carry

    lax.fori_loop(0, Y, pack, 0)

    pl.semaphore_wait(barrier, PEERS - 1 + 24)

    def drain(ref, start, count, sem):
        pltpu.make_async_copy(ref.at[pl.ds(start, count)], ref.at[pl.ds(start, count)], sem).wait()

    def send_quarter(src, dst_ref, i, out_sem, in_sem):
        def send(k, carry):
            peer = chan_of(my_y + i, far_first(k // 2), my_c + k % 2)

            @pl.when(peer != me)
            def _():
                pltpu.make_async_remote_copy(
                    src.at[peer], dst_ref.at[me], out_sem, in_sem.at[i],
                    device_id={"chan": peer}, device_id_type=MESH,
                ).start()
            return carry

        lax.fori_loop(0, 32, send, 0)

    def came_from(i):
        return lax.rem(my_y + Y - i, Y)

    def wait_quarter(ref, i, sem):
        @pl.when(i == 0)
        def _():
            drain(ref, 0, 31, sem.at[i])

        @pl.when(i > 0)
        def _():
            drain(ref, came_from(i) * 32, 32, sem.at[i])

    def note_line(k, carry):
        z = lax.rem(my_z + k, Z)
        pltpu.make_async_remote_copy(
            note.at[z], line_note.at[my_z], note_send, note_recv,
            device_id={"chan": chan_of(my_y, z, my_c)}, device_id_type=MESH,
        ).start()
        return carry

    lax.fori_loop(1, Z, note_line, 0)
    line_note[pl.ds(my_z, 1)] = note[pl.ds(my_z, 1)]
    got[pl.ds(me, 1)] = sent[pl.ds(me, 1)]
    send_quarter(sent, got, 0, send_sem, recv_sem)
    drain(line_note, 0, Z - 1, note_recv)

    def note_plane(k, carry):
        other = lax.rem(spot + k, 8)
        pltpu.make_async_remote_copy(
            line_note, got_note.at[spot], pass_send, pass_recv,
            device_id={"chan": chan_of(other // 2, my_z, other % 2)}, device_id_type=MESH,
        ).start()
        return carry

    lax.fori_loop(1, 8, note_plane, 0)

    def send_rest(i, carry):
        send_quarter(sent, got, i, send_sem, recv_sem)
        return carry

    lax.fori_loop(1, Y, send_rest, 0)
    got_note[pl.ds(spot, 1)] = line_note[...].reshape(1, Z, 1, 128)

    column[...] = as_column(pp_ref[...])
    sc_g[...] = (column[:, 0:1] * gm[...].astype(FULL)).astype(HALF)
    sc_h[...] = (column[:, 0:1] * hm[...].astype(FULL)).astype(HALF)

    def climb(i, trace):
        rows = at(i, PART)
        part = dot(gm[rows, :], sc_h[...]) - dot(hm[rows, :], sc_g[...])
        flow_ref[rows, :] = 0.5 * part
        on = iota((PART, CAP), 0) + i * PART == iota((PART, CAP), 1)
        return trace + jnp.sum(jnp.where(on, part, 0.0), axis=0, keepdims=True)

    trace = lax.fori_loop(0, CAP // PART, climb, jnp.zeros((1, CAP), FULL))
    trace = jnp.broadcast_to(jnp.sum(trace, axis=1, keepdims=True), (1, 128))
    plane_sum[pl.ds(seat, 1)] = trace.reshape(1, 1, 128)

    def share(k, carry):
        @pl.when(k != seat)
        def _():
            pltpu.make_async_remote_copy(
                plane_sum.at[seat], plane_sum.at[seat], plane_send, plane_recv,
                device_id={"chan": chan_of((k // 2) % 4, my_z, k % 2), "grp": k // 8},
                device_id_type=MESH,
            ).start()
        return carry

    lax.fori_loop(0, PLANE, share, 0)

    moved = iota((CAP, CAP), 0) == cols_ref[...]
    mix_g[...] = one_hot(moved)
    scale = jnp.sum(jnp.where(moved, ph_ref[...], 0.0), axis=1, keepdims=True)
    column[...] = jnp.broadcast_to(scale, (CAP, 128))
    swapped = iota((CAP, CAP), 0) == swap_ref[...]
    mix_h[...] = one_hot(swapped & (iota((CAP, CAP), 1) < size))
    row = iota((CAP, 1), 0)
    dst_own = as_column(dst)[:, 0:1].astype(jnp.int32)
    dst_pair = jnp.sum(jnp.where(swapped, dst, 0.0), axis=1, keepdims=True).astype(jnp.int32)
    dst_own = jnp.where(row < size, dst_own, -1)
    dst_pair = jnp.where(row < size, dst_pair, -1)

    def route_back(q, carry):
        spots = iota((CAP, STEP), 1) + q * STEP
        own = jnp.where(spots == dst_own, 1.0, 0.0)
        backward[q] = (own - jnp.where(spots == dst_pair, 1.0, 0.0)).astype(HALF)
        return carry

    lax.fori_loop(0, Y, route_back, 0)
    acc[...] = jnp.zeros((2 * CAP, CAP), FULL)

    drain(got_note, 0, 7, pass_recv)
    flat = got_note[...].reshape(PEERS, 128).astype(HALF)
    r_peer = iota((PEERS, ROWS), 1) // LINES
    r_seat = (r_peer // 32 * 2 + r_peer % 2) * Z + (r_peer // 2) % Z
    r_slot = iota((PEERS, ROWS), 1) // STRIP % SLOTS
    placed = jnp.zeros((16, ROWS), FULL)
    for t in range(SLOTS):
        pick = one_hot(iota((16, 128), 1) == SLOTS * spot + t)
        by_peer = dot_t(pick, flat).astype(HALF)
        placed += dot(by_peer, one_hot((r_seat == iota((PEERS, ROWS), 0)) & (r_slot == t)))
    source[...] = 4 * (placed[0:1, :].astype(jnp.int32) - 1) + iota((1, ROWS), 1) % STRIP

    def route(q, carry):
        pick = one_hot(iota((CAP, STEP), 0) == source[:, at(q, STEP)])
        forward[q] = dot(mix_g[...], pick).astype(HALF)
        return carry

    lax.fori_loop(0, Y, route, 0)

    def arrive(i, carry):
        wait_quarter(got, i, recv_sem)
        q = came_from(i)
        block = got[pl.ds(q * 32, 32)].astype(FULL)
        g = block[:, 0:LINES, :].reshape(STEP, CAP).astype(HALF)
        h = block[:, LINES:, :].reshape(STEP, CAP).astype(HALF)
        left_g[at(q, STEP), :] = g
        left_h[at(q, STEP), :] = h
        acc[0:CAP, :] += dot(forward[q], g)
        acc[CAP:, :] += dot(forward[q], h)
        return carry

    lax.fori_loop(0, Y, arrive, 0)
    sc_g[...] = (column[:, 0:1] * acc[0:CAP, :]).astype(HALF)
    sc_h[...] = (column[:, 0:1] * acc[CAP:, :]).astype(HALF)

    def along(k, carry):
        pltpu.make_async_remote_copy(
            line_sum.at[my_z], line_sum.at[my_z], line_send, line_recv,
            device_id={"chan": chan_of(my_y, my_z + k, my_c)}, device_id_type=MESH,
        ).start()
        return carry

    def finish(i, carry):
        quarter = lax.rem(my_y + i, Y)
        rows = at(quarter, STEP)
        part = dot(left_g[rows, :], sc_h[...]) - dot(left_h[rows, :], sc_g[...])
        ret[pl.ds(quarter * 32, 32)] = part.reshape(32, LINES, CAP).astype(HALF)
        send_quarter(ret, got_ret, i, ret_send, ret_recv)

        @pl.when(i == 0)
        def _():
            drain(plane_sum, 0, PLANE - 1, plane_recv)
            drain(plane_sum, 0, PLANE - 1, plane_send)
            line_sum[pl.ds(my_z, 1)] = jnp.sum(plane_sum[...], axis=0, keepdims=True)
            lax.fori_loop(1, Z, along, 0)
        return carry

    lax.fori_loop(0, Y, finish, 0)
    got_ret[pl.ds(me, 1)] = ret[pl.ds(me, 1)]

    drain(note, 0, Z - 1, note_send)
    drain(got_note, 0, 7, pass_send)
    drain(sent, 0, PEERS - 1, send_sem)

    def fold(i, carry):
        wait_quarter(got_ret, i, ret_recv)
        q = came_from(i)
        block = got_ret[pl.ds(q * 32, 32)].astype(FULL).reshape(STEP, CAP).astype(HALF)
        swap = dot(block, mix_h[...]).astype(HALF)
        kept = jnp.where(iota((STEP, CAP), 1) < size, block.astype(FULL), 0.0).astype(HALF)
        flow_ref[...] += dot(backward[q], kept) - dot(backward[q], swap)
        return carry

    lax.fori_loop(0, Y, fold, 0)
    drain(line_sum, 0, Z - 1, line_recv)
    energy_ref[...] = 0.25 * jnp.sum(line_sum[...], axis=0)
    drain(ret, 0, PEERS - 1, ret_send)
    drain(line_sum, 0, Z - 1, line_send)


def on_device(eta, ham, pp, ph, size, dev, sub, cols, swap):
    vmem = pl.BlockSpec(memory_space=pltpu.VMEM)
    hbm = pl.BlockSpec(memory_space=pl.ANY)
    dma = pltpu.SemaphoreType.DMA
    half = lambda *s: pltpu.VMEM(s, HALF)
    full = lambda *s: pltpu.VMEM(s, FULL)
    flow, energy = pl.pallas_call(
        kernel,
        out_shape=(
            jax.ShapeDtypeStruct((CAP, CAP), FULL),
            jax.ShapeDtypeStruct((1, 128), FULL),
        ),
        in_specs=[pl.BlockSpec(memory_space=pltpu.SMEM), hbm, hbm] + [vmem] * 6,
        out_specs=(vmem, vmem),
        scratch_shapes=[
            half(CAP, CAP), half(CAP, CAP),
            half(PEERS, 2 * LINES, CAP), full(Z, 1, 128),
            half(PEERS, 2 * LINES, CAP), full(Z, 1, 128), full(Y * CORES, Z, 1, 128),
            half(ROWS, CAP), half(ROWS, CAP),
            half(CAP, CAP), half(CAP, CAP), half(CAP, CAP), half(CAP, CAP),
            half(Y, CAP, STEP), half(Y, CAP, STEP), full(2 * CAP, CAP),
            half(PEERS, LINES, CAP), half(PEERS, LINES, CAP),
            full(CAP, 128), pltpu.VMEM((1, ROWS), jnp.int32),
            full(PLANE, 1, 128), full(Z, 1, 128),
            dma((2,)), dma, dma((Y,)), dma, dma, dma, dma, dma, dma((Y,)), dma, dma, dma, dma,
        ],
        compiler_params=pltpu.CompilerParams(
            collective_id=0, has_side_effects=True, vmem_limit_bytes=60 << 20
        ),
    )(size, eta[0], ham[0], pp, ph, dev, sub, cols, swap)
    return flow[None], energy[0, 0]


def solution(mesh):
    return jax.shard_map(
        on_device,
        mesh=mesh,
        in_specs=(
            P(AXES, None, None), P(AXES, None, None), P(AXES, None), P(AXES, None), P(AXES),
            P(AXES, None), P(AXES, None), P(AXES, None), P(AXES, None),
        ),
        out_specs=(P(AXES, None, None), P()),
        check_vma=False,
    )
```
